32 devices in a mesh: groups: 2 (over y), expert: 8 (over z, core), dp: 2 (over x).
Axes of the slice: x: 2, y: 2, z: 4, core: 2. Of those that a mesh axis runs over, the one named last changes fastest.
Arguments:
- tokens: bfloat16 [1024, 2048], P(('groups', 'expert'), 'dp'), parts along dimension 0, may hold values from -6 to 6
- expert_ids: int32 [1024, 8], P(('groups', 'expert')), parts along dimension 0, may hold values from 0 to 15, all different within a row; in each aligned block of 64 rows (0 to 63, 64 to 127, ...) at most 64 rows name the same one
- gate_levels: int32 [1024, 8], P(('groups', 'expert')), parts along dimension 0, may hold values from 1 to 255
- gate_weight: bfloat16 [16, 2048, 1536], P('expert', None, 'dp'), may hold values from -0.125 to 0.125
- up_weight: bfloat16 [16, 2048, 1536], P('expert', None, 'dp'), may hold values from -0.125 to 0.125
- down_weight: bfloat16 [16, 1536, 2048], P('expert', None, 'dp'), may hold values from -0.15625 to 0.15625
Outputs:
- mixed: bfloat16 [1024, 2048], P(('groups', 'expert'), 'dp'), parts along dimension 0
The draws below stay inside these ranges and needn't reach their ends.
There are 2 independent parts, one for each index of `groups`. The reference program is written for one: setup_inputs(seed, part) draws one part's arguments, and reference() takes and returns one part's arrays. A program takes and returns all parts, laid end to end along the dimension named above; an argument that names none is the same for every part. Nothing has to cross between parts.
Inputs may be any that keep to these rules, and one draw needn't show every extreme that they name: `expert_ids`: each row names 8 different experts. Among the rows of one index of the expert axis no expert is named more than 64 times, a bound that some block reaches.
All inputs are finite; a program needn't handle non-finite values.
Results may differ from the reference program's by a relative error of at most 0.0057.
Values may be sent and summed in bfloat16 or wider, within the bound.
A program may use at most 64 MiB of HBM per device.

```python
import math
import jax
import jax.numpy as jnp
import numpy as np
from jax import lax

D = 2048
FF = 1536
TOP = 8
TOK_DEV = 64
EXPERTS = 16
TOKENS = 512
CAP = 64
N_EXPERT = 8


def with_ends(drawn, key, least, top_value):
    longest = drawn.shape.index(max(drawn.shape))
    spots = []
    for shift in (0, 1):
        where = [jax.random.randint(jax.random.fold_in(key, axis), (), 0, length) for axis, length in enumerate(drawn.shape)]
        where[longest] = (where[longest] + shift) % drawn.shape[longest]
        spots.append(tuple(where))
    return drawn.at[spots[0]].set(least).at[spots[1]].set(top_value)


def level_of(own_key, dims, split, least, largest):
    def one(dim, blocks):
        steps = jax.random.uniform(jax.random.fold_in(jax.random.fold_in(own_key, 6), dim), (blocks,), jnp.float32, least / len(split), largest / len(split))
        return jnp.repeat(jnp.exp(steps), dims[dim] // blocks).reshape((-1,) + (1,) * (len(dims) - dim - 1))

    level = one(*split[0])
    for cut in split[1:]:
        level = level * one(*cut)
    return level


def routed_block(key, own, number, rows, number_of, top, bound, skew):
    ranking = jax.random.permutation(key, number_of)
    packed, usual = load_shares(number_of, rows * top, bound, skew, True), load_shares(number_of, rows * top, bound, skew, False)
    places = jnp.arange(number_of)

    def named(lengths, turn):
        used = int((lengths > 0).sum())
        fixed = max(1, used // 4)
        shifted = fixed + (places - fixed + turn * (used - fixed)) % max(1, number_of - fixed)
        return jnp.zeros((number_of,), jnp.int32).at[ranking[jnp.where(places < fixed, places, shifted)]].set(jnp.asarray(lengths, jnp.int32))

    lengths = jnp.where(number % 4 == 0, named(packed, number // 4), named(usual, number - number // 4 - 1))
    mixed = jax.random.permutation(jax.random.fold_in(own, 3), number_of)
    donor, sink = mixed[0:number_of // 2 * 2:2], mixed[1:number_of // 2 * 2:2]
    slack = jnp.minimum(lengths[donor] - 1, bound - lengths[sink]) // 2
    slack = jnp.where((donor == ranking[0]) | (sink == ranking[0]) | (lengths[sink] == 0), 0, jnp.maximum(slack, 0))
    shifted = jax.random.randint(jax.random.fold_in(own, 4), (number_of // 2,), 0, 1 << 20) % (slack + 1)
    lengths = lengths.at[donor].add(-shifted).at[sink].add(shifted)
    members = jnp.searchsorted(jnp.cumsum(lengths), jnp.arange(rows * top), side="right").astype(jnp.int32)
    grid = members.reshape(top, rows).T
    grid = grid[jax.random.permutation(jax.random.fold_in(own, 1), rows)]
    turn = jax.random.randint(jax.random.fold_in(own, 2), (rows, 1), 0, top)
    return jnp.take_along_axis(grid, (jnp.arange(top)[None, :] + turn) % top, axis=1)


def load_shares(amount, total, most, lean, full):
    weights = [(1 << 20) // math.isqrt(grade ** lean) + 1 for grade in range(1, amount + 1)]
    largest = most if full else min(most, max(-(-total // amount), total * weights[0] // sum(weights)))
    least = 1 if total - largest >= amount - 1 else 0
    given, rest = [largest] + [least] * (amount - 1), total - largest - least * (amount - 1)
    while rest > 0:
        candidates = [i for i in range(1, amount) if given[i] < largest] or [i for i in range(1, amount) if given[i] < most]
        mass, budget = sum([weights[i] for i in candidates]), rest
        for i in candidates:
            extra = min(most - given[i], max(1, budget * weights[i] // mass), rest)
            given[i] = given[i] + extra
            rest = rest - extra
    return np.array(given)


def bell_draw(key, shape, scale, reach, split=(), kind=jnp.bfloat16):
    array = jax.random.normal(key, shape, jnp.float32) * scale
    if len(split) > 0:
        array = level_of(key, shape, split, -0.22, 0.18) * array
    return jnp.clip(array, min=-reach, max=reach).astype(kind)


def setup_inputs(seed: int = 0, part: int = 0) -> dict:
    arg_keys = jax.random.split(jax.random.key(seed), 7)
    own_keys = jax.random.split(jax.random.fold_in(arg_keys[6], part), 7)
    tokens = bell_draw(own_keys[0], (TOKENS, D), 1.0, 6.0, ((0, 8), (1, 2)))
    expert_ids_keys = jax.random.split(jax.random.fold_in(own_keys[1], 1), TOKENS // TOK_DEV)
    expert_ids_turns = jax.random.permutation(jax.random.fold_in(own_keys[1], 3), TOKENS // TOK_DEV)
    expert_ids = jax.vmap(lambda own, number: routed_block(jax.random.fold_in(own_keys[1], 2), own, number, TOK_DEV, EXPERTS, TOP, CAP, 2))(expert_ids_keys, expert_ids_turns).reshape((TOKENS, TOP))
    gate_levels = with_ends(jax.random.randint(own_keys[2], (TOKENS, TOP), 1, 256), jax.random.fold_in(own_keys[2], 1), 1, 255).astype(jnp.int32)
    gate_weight = bell_draw(arg_keys[3], (EXPERTS, D, FF), D ** -0.5, 0.125, ((0, 8), (2, 2)))
    up_weight = bell_draw(arg_keys[4], (EXPERTS, D, FF), D ** -0.5, 0.125, ((0, 8), (2, 2)))
    down_weight = bell_draw(arg_keys[5], (EXPERTS, FF, D), FF ** -0.5, 0.15625, ((0, 8), (2, 2)))
    return dict(tokens=tokens, expert_ids=expert_ids, gate_levels=gate_levels, gate_weight=gate_weight, up_weight=up_weight, down_weight=down_weight)


def reference(tokens, expert_ids, gate_levels, gate_weight, up_weight, down_weight):
    shares = gate_levels.astype(jnp.float32) / 256.0
    row_limit = N_EXPERT * CAP
    count_tokens = tokens.shape[0]

    def per_expert(running, expert_index):
        matched = expert_ids == expert_index
        weight_sum = jnp.sum(jnp.where(matched, shares, jnp.float32(0.0)), axis=1)
        chosen = jnp.any(matched, axis=1)
        token_rows = jnp.nonzero(chosen, size=row_limit, fill_value=0)[0].astype(jnp.int32)
        picked = tokens[token_rows]
        gate_part = jnp.dot(picked, gate_weight[expert_index], preferred_element_type=jnp.float32)
        up_part = jnp.dot(picked, up_weight[expert_index], preferred_element_type=jnp.float32)
        hidden = (jax.nn.silu(gate_part) * up_part).astype(jnp.bfloat16)
        expert_out = jnp.dot(hidden, down_weight[expert_index], preferred_element_type=jnp.float32).astype(jnp.bfloat16)
        filled = jnp.arange(row_limit, dtype=jnp.int32) < jnp.sum(chosen.astype(jnp.int32))
        factor = jnp.where(filled, weight_sum[token_rows], jnp.float32(0.0))
        running = running.at[token_rows].add(factor[:, None] * expert_out.astype(jnp.float32))
        return running, None

    start_sum = jnp.zeros((count_tokens, tokens.shape[1]), jnp.float32)
    labels = jnp.arange(gate_weight.shape[0], dtype=jnp.int32)
    total_sum, unused = lax.scan(per_expert, start_sum, labels)
    return total_sum.astype(jnp.bfloat16)
```

```python
import functools

import jax
import jax.numpy as jnp
from jax import lax
from jax.experimental import pallas as pl
from jax.experimental.pallas import tpu as pltpu
from jax.sharding import PartitionSpec as P

MESH = pl.DeviceIdType.MESH
WIDE = 256


def slot_numbers(chosen_ids, experts, capacity):
    flat_ids = chosen_ids.reshape(-1)
    labels = jnp.arange(experts, dtype=jnp.int32)
    onehot = (flat_ids[:, None] == labels[None, :]).astype(jnp.int32)
    before = jnp.cumsum(onehot, axis=0) - onehot
    position = jnp.sum(before * onehot, axis=1)
    return (flat_ids * capacity + position).reshape(chosen_ids.shape)


def route_matrix(slots, count):
    targets = jnp.arange(count, dtype=jnp.int32)
    return jnp.any(targets[:, None, None] == slots[None, :, :], axis=2).astype(jnp.bfloat16)


def routed_on_device(tokens, expert_ids, gate_levels, gate_weight, up_weight, down_weight):
    tok_dev = tokens.shape[0]
    picks = expert_ids.shape[1]
    exp_dev = gate_weight.shape[0]
    n_expert = lax.axis_size("expert")
    experts = exp_dev * n_expert
    capacity = min(tok_dev, max(2, 2 * tok_dev * picks // experts))
    slot_count = experts * capacity
    own_slots = slot_numbers(expert_ids, experts, capacity)
    route = route_matrix(own_slots, slot_count)
    whole = lax.all_gather(tokens, "dp", axis=1, tiled=True)
    outgoing = jnp.dot(route, whole, preferred_element_type=jnp.float32).astype(jnp.bfloat16)
    outgoing = outgoing.reshape(n_expert, exp_dev, capacity, whole.shape[1])
    arrived = lax.all_to_all(outgoing, "expert", split_axis=0, concat_axis=0, tiled=True)
    gate_part = jnp.einsum(
        "sxcd,xdf->sxcf", arrived, gate_weight, preferred_element_type=jnp.float32
    )
    up_part = jnp.einsum("sxcd,xdf->sxcf", arrived, up_weight, preferred_element_type=jnp.float32)
    hidden = (jax.nn.silu(gate_part) * up_part).astype(jnp.bfloat16)
    out_features = down_weight.shape[2]
    outputs = jnp.einsum(
        "sxcf,xfk->sxck",
        lax.all_gather(hidden, "dp", axis=3, tiled=True),
        down_weight,
        preferred_element_type=jnp.float32,
    )
    result = outputs.astype(jnp.bfloat16)
    returned = lax.all_to_all(result, "expert", split_axis=0, concat_axis=0, tiled=True)
    returned = returned.reshape(slot_count, out_features)
    shares = gate_levels.astype(jnp.float32) / 256.0
    targets = jnp.arange(slot_count, dtype=jnp.int32)
    weighting = jnp.sum(
        jnp.where(
            targets[None, :, None] == own_slots[:, None, :], shares[:, None, :], jnp.float32(0.0)
        ),
        axis=2,
    )
    weighting = weighting.astype(jnp.bfloat16)
    combined = jnp.dot(weighting, returned, preferred_element_type=jnp.float32)
    return combined.astype(jnp.bfloat16)


def near_first(chips):
    return [sorted(range(chips), key=lambda q: (abs(q - z), q if 2 * z < chips else -q)) for z in range(chips)]


def dense_kernel(
    chips, tok, ids, levels, gate_hbm, up_hbm, down_hbm, out,
    gate_w, up_w, down_w, x_buf, s_buf, hid, part, pair_out, pair_in, ret_out, ret_in, total,
    w_sem, x_send, x_recv, t_send, h_send, h_recv, p_send, p_recv, r_send, r_recv,
):
    e = lax.axis_index("expert")
    d = lax.axis_index("dp")
    z, c = lax.div(e, 2), lax.rem(e, 2)
    rows = tok.shape[0]
    exp_dev, depth, ff = gate_w.shape
    half = depth // 2
    width = down_w.shape[2]
    mate = z * 2 + 1 - c

    loads = []
    for x in range(exp_dev):
        for i, (source, held) in enumerate(((gate_hbm, gate_w), (up_hbm, up_w))):
            loads.append(pltpu.make_async_copy(source.at[x], held.at[x], w_sem.at[x, i]))
    for x in range(exp_dev):
        loads.append(pltpu.make_async_copy(down_hbm.at[x], down_w.at[x], w_sem.at[x, 2]))
    for load in loads:
        load.start()

    barrier = pltpu.get_barrier_semaphore()
    pl.semaphore_signal(barrier, inc=1, device_id={"dp": 1 - d}, device_id_type=MESH)
    pl.semaphore_signal(barrier, inc=1, device_id={"expert": mate}, device_id_type=MESH)
    for i in range(1, chips):
        pl.semaphore_signal(
            barrier, inc=1, device_id={"expert": lax.rem(z + i, chips) * 2 + c}, device_id_type=MESH
        )

    own_rows = pl.ds(pl.multiple_of(c * rows, rows), rows)
    lane = lax.broadcasted_iota(jnp.int32, (rows, 128), 1)
    share = jnp.zeros((rows, 128), jnp.float32)
    for k in range(ids.shape[1]):
        level = levels[:, k : k + 1].astype(jnp.float32) / 256.0
        share = share + jnp.where(ids[:, k : k + 1] == lane, level, 0.0)
    s_buf[z, own_rows, :] = share.astype(s_buf.dtype)
    x_buf[z, d, own_rows, :] = tok[...]
    pl.semaphore_wait(barrier, chips + 1)

    def unit(q, core, j):
        at = pl.ds(pl.multiple_of(core * rows, rows), rows)
        if isinstance(j, int) and j == 2:
            return s_buf.at[q, at]
        return x_buf.at[q, j, at]

    def swap():
        return pltpu.make_async_remote_copy(
            src_ref=tok, dst_ref=unit(z, c, d), send_sem=t_send, recv_sem=x_recv.at[z, c, d],
            device_id={"dp": 1 - d}, device_id_type=MESH,
        )

    def forward(q, j, way):
        target = (mate, e + 2, e - 2)[way]
        return pltpu.make_async_remote_copy(
            src_ref=unit(q, c, j), dst_ref=unit(q, c, j),
            send_sem=x_send.at[q, j, way], recv_sem=x_recv.at[q, c, j],
            device_id={"expert": target}, device_id_type=MESH,
        )

    def arrived(q, core, j):
        pltpu.make_async_remote_copy(
            src_ref=unit(q, core, j), dst_ref=unit(q, core, j),
            send_sem=t_send, recv_sem=x_recv.at[q, core, j],
            device_id={"expert": mate}, device_id_type=MESH,
        ).wait_recv()

    def send_own(j, finish=False):
        for way, there in ((0, None), (1, z < chips - 1), (2, z > 0)):
            def go(way=way):
                copy = forward(z, j, way)
                copy.wait_send() if finish else copy.start()
            go() if there is None else pl.when(there)(go)

    def relay(step, finish=False):
        for way in (1, 2):
            q = z - step if way == 1 else z + step
            inside = z >= step if way == 1 else z + step < chips
            further = jnp.logical_and(inside, z < chips - 1) if way == 1 else jnp.logical_and(inside, z > 0)
            for j in (0, 1, 2):
                @pl.when(inside)
                def _(q=q, j=j):
                    if finish:
                        forward(q, j, 0).wait_send()
                    else:
                        arrived(q, c, j)

                @pl.when(further)
                def _(q=q, j=j, way=way):
                    copy = forward(q, j, way)
                    copy.wait_send() if finish else copy.start()

                if not finish:
                    @pl.when(inside)
                    def _(q=q, j=j):
                        forward(q, j, 0).start()

    swap().start()
    send_own(d)
    send_own(2)
    arrived(z, c, 1 - d)
    send_own(1 - d)

    table = near_first(chips)
    order = []
    for step in range(chips):
        q = jnp.int32(0)
        for place in range(chips):
            q = jnp.where(z == place, jnp.int32(table[place][step]), q)
        order.append(q)

    def cross(step, x):
        return pltpu.make_async_remote_copy(
            src_ref=hid.at[step, x, d], dst_ref=hid.at[step, x, d],
            send_sem=h_send.at[step, x], recv_sem=h_recv.at[step, x],
            device_id={"dp": 1 - d}, device_id_type=MESH,
        )

    def crossed(step, x):
        pltpu.make_async_remote_copy(
            src_ref=hid.at[step, x, 1 - d], dst_ref=hid.at[step, x, 1 - d],
            send_sem=h_send.at[step, x], recv_sem=h_recv.at[step, x],
            device_id={"dp": 1 - d}, device_id_type=MESH,
        ).wait_recv()

    def units(step):
        q = order[step]
        for j in (0, 1, 2):
            arrived(q, 1 - c, j)
        for x in range(exp_dev):
            if step == 0:
                loads[2 * x].wait()
                loads[2 * x + 1].wait()

            @pl.loop(0, ff // WIDE)
            def _(t):
                cols = pl.ds(pl.multiple_of(t * WIDE, WIDE), WIDE)
                low, high = x_buf[q, 0], x_buf[q, 1]
                gate = jnp.dot(low, gate_w[x, :half, cols], preferred_element_type=jnp.float32)
                gate = gate + jnp.dot(high, gate_w[x, half:, cols], preferred_element_type=jnp.float32)
                up = jnp.dot(low, up_w[x, :half, cols], preferred_element_type=jnp.float32)
                up = up + jnp.dot(high, up_w[x, half:, cols], preferred_element_type=jnp.float32)
                hid[step, x, d, :, cols] = (gate / (1.0 + jnp.exp(-gate)) * up).astype(hid.dtype)

            cross(step, x).start()

    def hand_over(step):
        return pltpu.make_async_remote_copy(
            src_ref=pair_out.at[step], dst_ref=pair_in.at[step],
            send_sem=p_send.at[step], recv_sem=p_recv.at[step],
            device_id={"expert": mate}, device_id_type=MESH,
        )

    def give_back(step):
        return pltpu.make_async_remote_copy(
            src_ref=ret_out.at[step], dst_ref=ret_in.at[z],
            send_sem=r_send.at[step], recv_sem=r_recv.at[z],
            device_id={"expert": order[step] * 2 + c}, device_id_type=MESH,
        )

    def outputs(step):
        q = order[step]
        lanes = lax.broadcasted_iota(jnp.int32, (2 * rows, 128), 1)
        for x in range(exp_dev):
            if step == 0:
                loads[2 * exp_dev + x].wait()
            picked = jnp.where(lanes == e * exp_dev + x, s_buf[q].astype(jnp.float32), 0.0)
            weight = jnp.sum(picked, axis=1, keepdims=True)
            crossed(step, x)

            @pl.loop(0, width // WIDE)
            def _(t):
                cols = pl.ds(pl.multiple_of(t * WIDE, WIDE), WIDE)
                res = jnp.dot(hid[step, x, 0], down_w[x, :ff, cols], preferred_element_type=jnp.float32)
                res = res + jnp.dot(hid[step, x, 1], down_w[x, ff:, cols], preferred_element_type=jnp.float32)
                res = res * weight
                for core in range(2):
                    piece = res[core * rows : (core + 1) * rows]
                    if x == 0:
                        part[core, :, cols] = piece
                    else:
                        part[core, :, cols] += piece

        pair_out[step] = part[1 - c].astype(pair_out.dtype)
        hand_over(step).start()
        hand_over(step).wait_recv()
        both = part[c] + pair_in[step].astype(jnp.float32)
        if step == 0:
            total[...] = both
        else:
            ret_out[step] = both.astype(ret_out.dtype)
            give_back(step).start()

    units(0)
    for step in range(1, chips):
        relay(step)
        units(step)
        outputs(step - 1)
    outputs(chips - 1)

    for i in range(1, chips):
        q = lax.rem(z + i, chips)
        pltpu.make_async_remote_copy(
            src_ref=ret_in.at[q], dst_ref=ret_in.at[q], send_sem=r_send.at[i], recv_sem=r_recv.at[q],
            device_id={"expert": mate}, device_id_type=MESH,
        ).wait_recv()
        if i < chips - 1:
            total[...] += ret_in[q].astype(jnp.float32)
        else:
            out[...] = (total[...] + ret_in[q].astype(jnp.float32)).astype(out.dtype)

    swap().wait_send()
    for j in (0, 1, 2):
        send_own(j, finish=True)
    for step in range(1, chips):
        relay(step, finish=True)
        give_back(step).wait_send()
    for step in range(chips):
        hand_over(step).wait_send()
        for x in range(exp_dev):
            cross(step, x).wait_send()


def dense_on_device(tokens, expert_ids, gate_levels, gate_weight, up_weight, down_weight):
    chips = lax.axis_size("expert") // 2
    rows, own = tokens.shape
    exp_dev, depth, ff = gate_weight.shape
    width = down_weight.shape[2]
    kind = tokens.dtype
    vmem = pl.BlockSpec(memory_space=pltpu.VMEM)
    anywhere = pl.BlockSpec(memory_space=pl.ANY)
    dma = pltpu.SemaphoreType.DMA
    flops = 2 * chips * 2 * rows * exp_dev * (2 * depth * ff + 2 * ff * width)
    return pl.pallas_call(
        functools.partial(dense_kernel, chips),
        out_shape=jax.ShapeDtypeStruct((rows, width), kind),
        in_specs=[vmem, vmem, vmem, anywhere, anywhere, anywhere],
        out_specs=vmem,
        scratch_shapes=[
            pltpu.VMEM(gate_weight.shape, kind),
            pltpu.VMEM(up_weight.shape, kind),
            pltpu.VMEM(down_weight.shape, kind),
            pltpu.VMEM((chips, 2, 2 * rows, own), kind),
            pltpu.VMEM((chips, 2 * rows, 128), kind),
            pltpu.VMEM((chips, exp_dev, 2, 2 * rows, ff), kind),
            pltpu.VMEM((2, rows, width), jnp.float32),
            pltpu.VMEM((chips, rows, width), kind),
            pltpu.VMEM((chips, rows, width), kind),
            pltpu.VMEM((chips, rows, width), kind),
            pltpu.VMEM((chips, rows, width), kind),
            pltpu.VMEM((rows, width), jnp.float32),
            dma((exp_dev, 3)),
            dma((chips, 3, 3)),
            dma((chips, 2, 3)),
            dma,
            dma((chips, exp_dev)),
            dma((chips, exp_dev)),
            dma((chips,)),
            dma((chips,)),
            dma((chips,)),
            dma((chips,)),
        ],
        compiler_params=pltpu.CompilerParams(
            collective_id=0, has_side_effects=True, vmem_limit_bytes=60 * 1024 * 1024
        ),
        cost_estimate=pl.CostEstimate(
            flops=flops, bytes_accessed=2 * 3 * gate_weight.size, transcendentals=0
        ),
    )(tokens, expert_ids, gate_levels, gate_weight, up_weight, down_weight)


def on_device(tokens, expert_ids, gate_levels, gate_weight, up_weight, down_weight):
    rows, own = tokens.shape
    exp_dev, depth, ff = gate_weight.shape
    n_expert = lax.axis_size("expert")
    width = down_weight.shape[2]
    experts = exp_dev * n_expert
    dense = (
        2 * rows * expert_ids.shape[1] >= rows * experts
        and lax.axis_size("dp") == 2
        and n_expert % 2 == 0
        and n_expert >= 4
        and experts <= 128
        and rows % 16 == 0
        and own % 128 == 0
        and ff % WIDE == 0
        and width % WIDE == 0
    )
    call = dense_on_device if dense else routed_on_device
    return call(tokens, expert_ids, gate_levels, gate_weight, up_weight, down_weight)


def solution(mesh):
    in_specs = (
        P(("groups", "expert"), "dp"),
        P(("groups", "expert"), None),
        P(("groups", "expert"), None),
        P("expert", None, "dp"),
        P("expert", None, "dp"),
        P("expert", None, "dp"),
    )
    out_specs = P(("groups", "expert"), "dp")
    return jax.shard_map(
        on_device, mesh=mesh, in_specs=in_specs, out_specs=out_specs, check_vma=False
    )
```

```python
import functools

import jax
import jax.numpy as jnp
from jax import lax
from jax.experimental import pallas as pl
from jax.experimental.pallas import tpu as pltpu
from jax.sharding import PartitionSpec as P

MESH = pl.DeviceIdType.MESH
WIDE = 256


def slot_numbers(chosen_ids, experts, capacity):
    flat_ids = chosen_ids.reshape(-1)
    labels = jnp.arange(experts, dtype=jnp.int32)
    onehot = (flat_ids[:, None] == labels[None, :]).astype(jnp.int32)
    before = jnp.cumsum(onehot, axis=0) - onehot
    position = jnp.sum(before * onehot, axis=1)
    return (flat_ids * capacity + position).reshape(chosen_ids.shape)


def route_matrix(slots, count):
    targets = jnp.arange(count, dtype=jnp.int32)
    return jnp.any(targets[:, None, None] == slots[None, :, :], axis=2).astype(jnp.bfloat16)


def routed_on_device(tokens, expert_ids, gate_levels, gate_weight, up_weight, down_weight):
    tok_dev = tokens.shape[0]
    picks = expert_ids.shape[1]
    exp_dev = gate_weight.shape[0]
    n_expert = lax.axis_size("expert")
    experts = exp_dev * n_expert
    capacity = min(tok_dev, max(2, 2 * tok_dev * picks // experts))
    slot_count = experts * capacity
    own_slots = slot_numbers(expert_ids, experts, capacity)
    route = route_matrix(own_slots, slot_count)
    whole = lax.all_gather(tokens, "dp", axis=1, tiled=True)
    outgoing = jnp.dot(route, whole, preferred_element_type=jnp.float32).astype(jnp.bfloat16)
    outgoing = outgoing.reshape(n_expert, exp_dev, capacity, whole.shape[1])
    arrived = lax.all_to_all(outgoing, "expert", split_axis=0, concat_axis=0, tiled=True)
    gate_part = jnp.einsum(
        "sxcd,xdf->sxcf", arrived, gate_weight, preferred_element_type=jnp.float32
    )
    up_part = jnp.einsum("sxcd,xdf->sxcf", arrived, up_weight, preferred_element_type=jnp.float32)
    hidden = (jax.nn.silu(gate_part) * up_part).astype(jnp.bfloat16)
    out_features = down_weight.shape[2]
    outputs = jnp.einsum(
        "sxcf,xfk->sxck",
        lax.all_gather(hidden, "dp", axis=3, tiled=True),
        down_weight,
        preferred_element_type=jnp.float32,
    )
    result = outputs.astype(jnp.bfloat16)
    returned = lax.all_to_all(result, "expert", split_axis=0, concat_axis=0, tiled=True)
    returned = returned.reshape(slot_count, out_features)
    shares = gate_levels.astype(jnp.float32) / 256.0
    targets = jnp.arange(slot_count, dtype=jnp.int32)
    weighting = jnp.sum(
        jnp.where(
            targets[None, :, None] == own_slots[:, None, :], shares[:, None, :], jnp.float32(0.0)
        ),
        axis=2,
    )
    weighting = weighting.astype(jnp.bfloat16)
    combined = jnp.dot(weighting, returned, preferred_element_type=jnp.float32)
    return combined.astype(jnp.bfloat16)


def visit_order(chips):
    table = []
    for z in range(chips):
        near = sorted(range(chips), key=lambda q: (abs(q - z), q if 2 * z < chips else -q))
        if 0 < z < chips - 1:
            near = near[:1] + near[2:] + near[1:2]
        else:
            near = near[:-2] + [near[-1], near[-2]]
        table.append(near)
    return table


def dense_kernel(
    chips, tok_hbm, ids_hbm, levels_hbm, gate_hbm, up_hbm, down_hbm, out,
    ids, levels, gate_w, up_w, down_w, x_buf, s_buf, hid, part, pair_out, pair_in, ret_out, ret_in, total,
    i_sem, w_sem, x_send, x_recv, t_send, h_send, h_recv, p_send, p_recv, r_send, r_recv,
):
    e = lax.axis_index("expert")
    d = lax.axis_index("dp")
    z, c = lax.div(e, 2), lax.rem(e, 2)
    rows = tok_hbm.shape[0]
    exp_dev, depth, ff = gate_w.shape
    half = depth // 2
    width = down_w.shape[2]
    mate = z * 2 + 1 - c

    barrier = pltpu.get_barrier_semaphore()
    pl.semaphore_signal(barrier, inc=1, device_id={"dp": 1 - d}, device_id_type=MESH)
    pl.semaphore_signal(barrier, inc=1, device_id={"expert": mate}, device_id_type=MESH)

    @pl.when(z > 0)
    def _():
        pl.semaphore_signal(barrier, inc=1, device_id={"expert": e - 2}, device_id_type=MESH)

    @pl.when(z < chips - 1)
    def _():
        pl.semaphore_signal(barrier, inc=1, device_id={"expert": e + 2}, device_id_type=MESH)

    mine = pl.ds(pl.multiple_of(c * rows, rows), rows)
    tok = x_buf.at[z, d, mine]
    tok_load = pltpu.make_async_copy(tok_hbm, tok, i_sem.at[0])
    ids_load = pltpu.make_async_copy(ids_hbm, ids, i_sem.at[1])
    levels_load = pltpu.make_async_copy(levels_hbm, levels, i_sem.at[2])
    for load in (tok_load, ids_load, levels_load):
        load.start()
    loads = []
    for x in range(exp_dev):
        for i, (source, held) in enumerate(((gate_hbm, gate_w), (up_hbm, up_w))):
            loads.append(pltpu.make_async_copy(source.at[x], held.at[x], w_sem.at[x, i]))
    for x in range(exp_dev):
        loads.append(pltpu.make_async_copy(down_hbm.at[x], down_w.at[x], w_sem.at[x, 2]))
    for load in loads:
        load.start()

    pl.semaphore_wait(barrier, 2 + jnp.minimum(z, 1) + jnp.minimum(chips - 1 - z, 1))

    tok_load.wait()

    def unit(q, core, j):
        at = pl.ds(pl.multiple_of(core * rows, rows), rows)
        if isinstance(j, int) and j == 2:
            return s_buf.at[q, at]
        return x_buf.at[q, j, at]

    def swap():
        return pltpu.make_async_remote_copy(
            src_ref=tok, dst_ref=unit(z, c, d), send_sem=t_send, recv_sem=x_recv.at[z, c, d],
            device_id={"dp": 1 - d}, device_id_type=MESH,
        )

    def forward(q, j, way):
        target = (mate, e + 2, e - 2)[way]
        return pltpu.make_async_remote_copy(
            src_ref=unit(q, c, j), dst_ref=unit(q, c, j),
            send_sem=x_send.at[q, j, way], recv_sem=x_recv.at[q, c, j],
            device_id={"expert": target}, device_id_type=MESH,
        )

    def arrived(q, core, j):
        pltpu.make_async_remote_copy(
            src_ref=unit(q, core, j), dst_ref=unit(q, core, j),
            send_sem=t_send, recv_sem=x_recv.at[q, core, j],
            device_id={"expert": mate}, device_id_type=MESH,
        ).wait_recv()

    def send_own(j, finish=False):
        for way, there in ((0, None), (1, z < chips - 1), (2, z > 0)):
            def go(way=way):
                copy = forward(z, j, way)
                copy.wait_send() if finish else copy.start()
            go() if there is None else pl.when(there)(go)

    def relay(step, finish=False):
        for way in (1, 2):
            q = z - step if way == 1 else z + step
            inside = z >= step if way == 1 else z + step < chips
            further = jnp.logical_and(inside, z < chips - 1) if way == 1 else jnp.logical_and(inside, z > 0)
            for j in (0, 1, 2):
                @pl.when(inside)
                def _(q=q, j=j):
                    if finish:
                        forward(q, j, 0).wait_send()
                    else:
                        arrived(q, c, j)

                @pl.when(further)
                def _(q=q, j=j, way=way):
                    copy = forward(q, j, way)
                    copy.wait_send() if finish else copy.start()

                if not finish:
                    @pl.when(inside)
                    def _(q=q, j=j):
                        forward(q, j, 0).start()

    swap().start()
    send_own(d)
    ids_load.wait()
    levels_load.wait()
    label = lax.broadcasted_iota(jnp.int32, (128, rows), 0)
    share = jnp.zeros((128, rows), jnp.float32)
    for k in range(ids.shape[0]):
        level = levels[k : k + 1, :].astype(jnp.float32) / 256.0
        share = share + jnp.where(ids[k : k + 1, :] == label, level, 0.0)
    s_buf[z, mine, :] = share.T.astype(s_buf.dtype)
    send_own(2)
    arrived(z, c, 1 - d)
    send_own(1 - d)

    table = visit_order(chips)
    order = []
    for step in range(chips):
        q = jnp.int32(0)
        for place in range(chips):
            q = jnp.where(z == place, jnp.int32(table[place][step]), q)
        order.append(q)

    def piece_of(step, x, side, t):
        return hid.at[step, x, side, :, pl.ds(pl.multiple_of(t * WIDE, WIDE), WIDE)]

    def cross(step, x, t):
        return pltpu.make_async_remote_copy(
            src_ref=piece_of(step, x, d, t), dst_ref=piece_of(step, x, d, t),
            send_sem=h_send.at[step, x, t], recv_sem=h_recv.at[step, x, t],
            device_id={"dp": 1 - d}, device_id_type=MESH,
        )

    def crossed(step, x, t):
        pltpu.make_async_remote_copy(
            src_ref=piece_of(step, x, 1 - d, t), dst_ref=piece_of(step, x, 1 - d, t),
            send_sem=h_send.at[step, x, t], recv_sem=h_recv.at[step, x, t],
            device_id={"dp": 1 - d}, device_id_type=MESH,
        ).wait_recv()

    def units(step):
        q = order[step]
        for j in (0, 1, 2):
            arrived(q, 1 - c, j)
        for x in range(exp_dev):
            if step == 0:
                loads[2 * x].wait()
                loads[2 * x + 1].wait()

            @pl.loop(0, ff // WIDE)
            def _(t):
                cols = pl.ds(pl.multiple_of(t * WIDE, WIDE), WIDE)
                low, high = x_buf[q, 0], x_buf[q, 1]
                gate = jnp.dot(low, gate_w[x, :half, cols], preferred_element_type=jnp.float32)
                gate = gate + jnp.dot(high, gate_w[x, half:, cols], preferred_element_type=jnp.float32)
                up = jnp.dot(low, up_w[x, :half, cols], preferred_element_type=jnp.float32)
                up = up + jnp.dot(high, up_w[x, half:, cols], preferred_element_type=jnp.float32)
                hid[step, x, d, :, cols] = (gate / (1.0 + jnp.exp(-gate)) * up).astype(hid.dtype)
                cross(step, x, t).start()


    def hand_over(step, t):
        return pltpu.make_async_remote_copy(
            src_ref=pair_out.at[step, t], dst_ref=pair_in.at[step, t],
            send_sem=p_send.at[step, t], recv_sem=p_recv.at[step, t],
            device_id={"expert": mate}, device_id_type=MESH,
        )

    def give_back(step, t):
        return pltpu.make_async_remote_copy(
            src_ref=ret_out.at[step, t], dst_ref=ret_in.at[z, t],
            send_sem=r_send.at[step, t], recv_sem=r_recv.at[z, t],
            device_id={"expert": order[step] * 2 + c}, device_id_type=MESH,
        )

    def outputs(step):
        q = order[step]
        lanes = lax.broadcasted_iota(jnp.int32, (2 * rows, 128), 1)
        for x in range(exp_dev):
            if step == 0:
                loads[2 * exp_dev + x].wait()
            picked = jnp.where(lanes == e * exp_dev + x, s_buf[q].astype(jnp.float32), 0.0)
            weight = jnp.sum(picked, axis=1, keepdims=True)
            for t in range(ff // WIDE):
                crossed(step, x, t)

            @pl.loop(0, width // WIDE)
            def _(t):
                cols = pl.ds(pl.multiple_of(t * WIDE, WIDE), WIDE)
                res = jnp.dot(hid[step, x, 0], down_w[x, :ff, cols], preferred_element_type=jnp.float32)
                res = res + jnp.dot(hid[step, x, 1], down_w[x, ff:, cols], preferred_element_type=jnp.float32)
                res = res * weight
                for core in range(2):
                    piece = res[core * rows : (core + 1) * rows]
                    if x == 0:
                        part[t, core] = piece
                    else:
                        part[t, core] += piece
                if x == exp_dev - 1:
                    pair_out[step, t] = part[t, 1 - c].astype(pair_out.dtype)
                    hand_over(step, t).start()

        for t in range(width // WIDE):
            hand_over(step, t).wait_recv()
            both = part[t, c] + pair_in[step, t].astype(jnp.float32)
            if step == 0:
                total[t] = both
            else:
                ret_out[step, t] = both.astype(ret_out.dtype)
                give_back(step, t).start()

    relayed = 0
    for step in range(chips):
        needed = max(abs(table[place][step] - place) for place in range(chips))
        while relayed < needed:
            relayed += 1
            relay(relayed)
        units(step)
        if step >= 1:
            if relayed + 1 < chips - 1:
                relayed += 1
                relay(relayed)
            outputs(step - 1)
    outputs(chips - 1)

    for i in range(1, chips):
        q = lax.rem(z + i, chips)
        for t in range(width // WIDE):
            pltpu.make_async_remote_copy(
                src_ref=ret_in.at[q, t], dst_ref=ret_in.at[q, t],
                send_sem=r_send.at[i, t], recv_sem=r_recv.at[q, t],
                device_id={"expert": mate}, device_id_type=MESH,
            ).wait_recv()
    for t in range(width // WIDE):
        full = total[t]
        for i in range(1, chips):
            full = full + ret_in[lax.rem(z + i, chips), t].astype(jnp.float32)
        out[:, t * WIDE : (t + 1) * WIDE] = full.astype(out.dtype)

    swap().wait_send()
    for j in (0, 1, 2):
        send_own(j, finish=True)
    for step in range(1, chips):
        relay(step, finish=True)
        for t in range(width // WIDE):
            give_back(step, t).wait_send()
    for step in range(chips):
        for t in range(width // WIDE):
            hand_over(step, t).wait_send()
        for x in range(exp_dev):
            for t in range(ff // WIDE):
                cross(step, x, t).wait_send()


def dense_on_device(tokens, expert_ids, gate_levels, gate_weight, up_weight, down_weight):
    chips = lax.axis_size("expert") // 2
    rows, own = tokens.shape
    exp_dev, depth, ff = gate_weight.shape
    width = down_weight.shape[2]
    kind = tokens.dtype
    tiles = width // WIDE
    picks = expert_ids.shape[1]
    vmem = pl.BlockSpec(memory_space=pltpu.VMEM)
    anywhere = pl.BlockSpec(memory_space=pl.ANY)
    dma = pltpu.SemaphoreType.DMA
    flops = 2 * chips * 2 * rows * exp_dev * (2 * depth * ff + 2 * ff * width)
    return pl.pallas_call(
        functools.partial(dense_kernel, chips),
        out_shape=jax.ShapeDtypeStruct((rows, width), kind),
        in_specs=[anywhere] * 6,
        out_specs=vmem,
        scratch_shapes=[
            pltpu.VMEM((picks, rows), jnp.int32),
            pltpu.VMEM((picks, rows), jnp.int32),
            pltpu.VMEM(gate_weight.shape, kind),
            pltpu.VMEM(up_weight.shape, kind),
            pltpu.VMEM(down_weight.shape, kind),
            pltpu.VMEM((chips, 2, 2 * rows, own), kind),
            pltpu.VMEM((chips, 2 * rows, 128), kind),
            pltpu.VMEM((chips, exp_dev, 2, 2 * rows, ff), kind),
            pltpu.VMEM((tiles, 2, rows, WIDE), jnp.float32),
            pltpu.VMEM((chips, tiles, rows, WIDE), kind),
            pltpu.VMEM((chips, tiles, rows, WIDE), kind),
            pltpu.VMEM((chips, tiles, rows, WIDE), kind),
            pltpu.VMEM((chips, tiles, rows, WIDE), kind),
            pltpu.VMEM((tiles, rows, WIDE), jnp.float32),
            dma((3,)),
            dma((exp_dev, 3)),
            dma((chips, 3, 3)),
            dma((chips, 2, 3)),
            dma,
            dma((chips, exp_dev, ff // WIDE)),
            dma((chips, exp_dev, ff // WIDE)),
            dma((chips, tiles)),
            dma((chips, tiles)),
            dma((chips, tiles)),
            dma((chips, tiles)),
        ],
        compiler_params=pltpu.CompilerParams(
            collective_id=0, has_side_effects=True, vmem_limit_bytes=67043328
        ),
        cost_estimate=pl.CostEstimate(
            flops=flops, bytes_accessed=2 * 3 * gate_weight.size, transcendentals=0
        ),
    )(tokens, expert_ids.T, gate_levels.T, gate_weight, up_weight, down_weight)


def on_device(tokens, expert_ids, gate_levels, gate_weight, up_weight, down_weight):
    rows, own = tokens.shape
    exp_dev, depth, ff = gate_weight.shape
    n_expert = lax.axis_size("expert")
    width = down_weight.shape[2]
    experts = exp_dev * n_expert
    dense = (
        2 * rows * expert_ids.shape[1] >= rows * experts
        and lax.axis_size("dp") == 2
        and n_expert % 2 == 0
        and n_expert >= 6
        and experts <= 128
        and rows % 16 == 0
        and own % 128 == 0
        and ff % WIDE == 0
        and width % WIDE == 0
    )
    call = dense_on_device if dense else routed_on_device
    return call(tokens, expert_ids, gate_levels, gate_weight, up_weight, down_weight)


def solution(mesh):
    in_specs = (
        P(("groups", "expert"), "dp"),
        P(("groups", "expert"), None),
        P(("groups", "expert"), None),
        P("expert", None, "dp"),
        P("expert", None, "dp"),
        P("expert", None, "dp"),
    )
    out_specs = P(("groups", "expert"), "dp")
    return jax.shard_map(
        on_device, mesh=mesh, in_specs=in_specs, out_specs=out_specs, check_vma=False
    )
```
